32 devices in a mesh: lat: 8 (over z, x), lev: 4 (over y, core).
Axes of the slice: x: 2, y: 2, z: 4, core: 2. Of those that a mesh axis runs over, the one named last changes fastest.
Arguments:
- pressure_thick: float32 [16, 192, 1152], P('lev', 'lat'), may hold values from 0.016 to 4.7
- potential_temp: float32 [16, 192, 1152], P('lev', 'lat'), may hold values from 0.5 to 3
- tracer: float32 [16, 192, 1152], P('lev', 'lat'), may hold values from 0 to 1
- east_courant: float32 [16, 192, 1152], P('lev', 'lat'), may hold values from -0.15 to 0.15
- north_courant: float32 [16, 192, 1152], P('lev', 'lat'), may hold values from -0.15 to 0.15
- polar_mask: int32 [192], P('lat'), may hold values from 0 to 1, as said below
- wave_cutoff: int32 [192], P('lat'), may hold values from 1 to 576, as said below
- level_weight: float32 [16], replicated, may hold values from 0.3 to 3
- target_surface: float32 [1], replicated, may hold values from 16 to 22.4
Outputs:
- remapped_thick: float32 [16, 192, 1152], P(None, 'lev', 'lat')
- remapped_temp: float32 [16, 192, 1152], P(None, 'lev', 'lat')
- remapped_tracer: float32 [16, 192, 1152], P(None, 'lev', 'lat')
The draws below stay inside these ranges and needn't reach their ends.
Inputs may be any that keep to these rules, and one draw needn't show every extreme that they name: `polar_mask`: 1 on the first and last P rows and 0 between, for one P from 24 to 38. `wave_cutoff`: rows with polar_mask 0 hold 576.
All inputs are finite; a program needn't handle non-finite values.
Results may differ from the reference program's by a relative error of at most 0.0003.
Values sent between devices are 32-bit elements; how exact they have to be, the bound alone decides.
A program may use at most 128 MiB of HBM per device.

```python
import math
import jax
import jax.numpy as jnp
from jax import lax

NLON = 1152
NLAT = 192
LEV = 16


def polar_caps(key):
    return jax.random.randint(jax.random.fold_in(key, 11), (), NLAT // 8, NLAT // 5 + 1)


def pole_distance():
    row_index = jnp.arange(NLAT, dtype=jnp.int32)
    return jnp.minimum(row_index, NLAT - 1 - row_index)


def draw_polar_mask(key, part):
    caps = polar_caps(key)
    return (pole_distance() < caps).astype(jnp.int32)


def draw_wave_cutoff(key, part):
    caps = polar_caps(key)
    distance = pole_distance()
    jitter = jax.random.randint(jax.random.fold_in(key, 13), (NLAT,), -2, 3)
    ramp = 1 + distance * (NLON // 2 - 1) // caps
    limited = jnp.clip(ramp + jitter, 1, NLON // 2)
    return jnp.where(distance < caps, limited, NLON // 2).astype(jnp.int32)


def draw_pressure_thick(key, part):
    height = jnp.arange(LEV, dtype=jnp.float32) / max(LEV - 1, 1)
    east_frac = jnp.arange(NLON, dtype=jnp.float32) / NLON
    north_frac = jnp.arange(NLAT, dtype=jnp.float32) / NLAT
    noise = jax.random.uniform(key, (LEV, NLAT, NLON), jnp.float32, 0.8, 1.2)
    lat_factor = 0.7 + 0.6 * north_frac
    base = 0.2 + 1.8 * height
    lon_factor = 0.5 + east_frac
    shape = base[:, None, None] * lat_factor[None, :, None] * lon_factor[None, None, :]
    return (shape * noise).astype(jnp.float32)


def levels(stream_key, extent, split, smallest, largest):
    factor_of = 1.0
    for dim, blocks in split:
        heights = jax.random.uniform(jax.random.fold_in(jax.random.fold_in(stream_key, 6), dim), (blocks,), jnp.float32, smallest / len(split), largest / len(split))
        factor_of = factor_of * jnp.repeat(jnp.exp(heights), extent[dim] // blocks).reshape((-1,) + (1,) * (len(extent) - 1 - dim))
    return factor_of


def setup_inputs(seed: int = 0) -> dict:
    streams_of = jax.random.split(jax.random.key(seed), 10)
    return {
        "pressure_thick": draw_pressure_thick(jax.random.fold_in(streams_of[9], 71), 0),
        "potential_temp": jnp.clip(0.5 + 2.5 * jax.random.uniform(streams_of[1], (LEV, NLAT, NLON), jnp.float32) ** levels(streams_of[1], (LEV, NLAT, NLON), ((0, 4), (1, 8)), -0.2, 0.2), 0.5, 3.0),
        "tracer": jnp.clip(1.0 * jax.random.uniform(streams_of[2], (LEV, NLAT, NLON), jnp.float32) ** levels(streams_of[2], (LEV, NLAT, NLON), ((0, 4), (1, 8)), -0.2, 0.2), 0.0, 1.0),
        "east_courant": jnp.clip(jax.random.uniform(streams_of[3], (LEV, NLAT, NLON), jnp.float32, -0.15, 0.15) * levels(streams_of[3], (LEV, NLAT, NLON), ((0, 4), (1, 8)), -0.4, 0.0), -0.15, 0.15),
        "north_courant": jnp.clip(jax.random.uniform(streams_of[4], (LEV, NLAT, NLON), jnp.float32, -0.15, 0.15) * levels(streams_of[4], (LEV, NLAT, NLON), ((0, 4), (1, 8)), -0.4, 0.0), -0.15, 0.15),
        "polar_mask": draw_polar_mask(jax.random.fold_in(streams_of[9], 71), 0),
        "wave_cutoff": draw_wave_cutoff(jax.random.fold_in(streams_of[9], 71), 0),
        "level_weight": jnp.clip(jnp.exp(jax.random.uniform(streams_of[7], (LEV,), jnp.float32, math.log(0.3), math.log(3.0))), 0.3, 3.0),
        "target_surface": jnp.clip(jax.random.uniform(streams_of[8], (1,), jnp.float32, 16.0, 22.4), 16.0, 22.4),
    }


def north_of(field):
    return jnp.pad(field, ((0, 0), (0, 1), (0, 0)))[:, 1:, :]


def south_of(field):
    return jnp.pad(field, ((0, 0), (1, 0), (0, 0)))[:, :-1, :]


def reference(pressure_thick, potential_temp, tracer, east_courant, north_courant, polar_mask, wave_cutoff, level_weight, target_surface):
    nlat = pressure_thick.shape[1]
    nlon = pressure_thick.shape[2]
    row_index = jnp.arange(nlat, dtype=jnp.float32)
    center_cos = jnp.sin((row_index + 0.5) * jnp.pi / nlat)
    face_cos = jnp.sin((row_index + 1.0) * jnp.pi / nlat)
    east_mass = east_courant * (pressure_thick + jnp.roll(pressure_thick, -1, axis=2)) * 0.5
    north_mass = north_courant * (pressure_thick + north_of(pressure_thick)) * 0.5 * face_cos[None, :, None]
    tendencies = []
    for scalar in (None, potential_temp, tracer):
        if scalar is None:
            east_part, north_part = east_mass, north_mass
        else:
            east_part = east_mass * (scalar + jnp.roll(scalar, -1, axis=2)) * 0.5
            north_part = north_mass * (scalar + north_of(scalar)) * 0.5
        diverge = (east_part - jnp.roll(east_part, 1, axis=2)) + (north_part - south_of(north_part)) / center_cos[None, :, None]
        tendencies.append(-diverge)
    wave = jnp.arange(nlon // 2 + 1, dtype=jnp.int32)
    keep = (polar_mask[:, None] > 0) & (wave[None, :] >= wave_cutoff[:, None])
    filtered = []
    for tendency in tendencies:
        spectrum = jnp.fft.rfft(tendency, axis=-1)
        high = jnp.fft.irfft(spectrum * keep[None, :, :], n=nlon, axis=-1)
        filtered.append(tendency - high.astype(tendency.dtype))
    new_thick = pressure_thick + filtered[0]
    new_temp = potential_temp + (filtered[1] - potential_temp * filtered[0]) / pressure_thick
    new_tracer = tracer + (filtered[2] - tracer * filtered[0]) / pressure_thick
    surface = jnp.sum(new_thick, axis=0)
    top_edge = jnp.cumsum(new_thick, axis=0) - new_thick
    share = level_weight / jnp.sum(level_weight)
    bound = surface[None] * jnp.cumsum(share)[:, None, None]

    def add_source(totals, source):
        thick_src, top_src, temp_src, tracer_src = source
        intersection = jnp.minimum(jnp.maximum(bound - top_src[None], 0.0), thick_src[None])
        return (totals[0] + temp_src[None] * intersection, totals[1] + tracer_src[None] * intersection), None

    zeros = jnp.zeros(bound.shape, jnp.float32)
    (cumul_temp, cumul_tracer), unused = lax.scan(add_source, (zeros, zeros), (new_thick, top_edge, new_temp, new_tracer))
    target_thick = surface[None] * share[:, None, None]
    remapped_temp = (cumul_temp - jnp.concatenate([zeros[:1], cumul_temp[:-1]], axis=0)) / target_thick
    remapped_tracer = (cumul_tracer - jnp.concatenate([zeros[:1], cumul_tracer[:-1]], axis=0)) / target_thick
    total = jnp.sum(new_thick * center_cos[None, :, None])
    mean_surface = total / (nlon * jnp.sum(center_cos))
    remapped_thick = target_thick * (target_surface[0] / mean_surface)
    return remapped_thick, remapped_temp, remapped_tracer
```

```python
import functools
import math

import jax
import jax.numpy as jnp
import numpy as np
from jax import lax
from jax.experimental import pallas as pl
from jax.experimental.pallas import tpu as pltpu
from jax.sharding import PartitionSpec as P

LANES = 128
SUB = 8
VMEM = pl.BlockSpec(memory_space=pltpu.VMEM)
SMEM = pl.BlockSpec(memory_space=pltpu.SMEM)
MESH = pl.DeviceIdType.MESH


@functools.cache
def dft_tables(nlon):
    radix = nlon // LANES
    b = np.arange(LANES)[:, None]
    k2 = np.arange(LANES)[None, :]
    high, low = [], []
    for k1 in range(radix // 2 + 1):
        phase = (b * (k1 + radix * k2) % nlon) * (2.0 * np.pi / nlon)
        c, s = np.cos(phase), np.sin(phase)
        table = np.block([[c, -s], [s, c]]).astype(np.float32)
        top = table.astype(jnp.bfloat16)
        high.append(top)
        low.append((table - top.astype(np.float32)).astype(jnp.bfloat16))
    return np.stack(high), np.stack(low)


@functools.cache
def row_tables(nlat):
    rows = np.arange(nlat, dtype=np.float64)
    out = np.zeros((nlat, LANES), np.float32)
    out[:, 0] = np.sin((rows + 0.5) * np.pi / nlat)
    out[:, 1] = 1.0 / np.sin((rows + 0.5) * np.pi / nlat)
    out[:, 2] = np.sin((rows + 1.0) * np.pi / nlat)
    out[:, 3] = np.sin(rows * np.pi / nlat)
    return out


def pack_plan(width, groups):
    full, rest = divmod(width, LANES)
    cap = LANES // rest if rest else 1
    tail_tiles = -(-groups // cap) if rest else 0
    return full, rest, cap, tail_tiles


def split_bf16(x):
    top = x.astype(jnp.bfloat16)
    return top, (x - top.astype(jnp.float32)).astype(jnp.bfloat16)


def update_kernel(
    n_lat,
    p_ref, t_ref, q_ref, e_ref, n_ref, south_ref, north_ref, mask_ref, cut_ref,
    rows_ref, mh_ref, ml_ref,
    send_ref, part_ref,
    tend, spec, new, yh, yl,
):
    levs, lats, nlon = p_ref.shape
    radix = nlon // LANES
    half = radix // 2
    first = pl.multiple_of(lax.axis_index("lat") * lats, SUB)
    table = rows_ref[pl.ds(first, lats), :]
    cc, icc, face, face_s = (table[:, c : c + 1] for c in range(4))
    face_s = face_s[0:1]
    row = lax.broadcasted_iota(jnp.int32, (lats, nlon), 0)

    def up(x, halo):
        return jnp.where(row == lats - 1, halo, pltpu.roll(x, lats - 1, 0))

    def down(x, halo):
        return jnp.where(row == 0, halo, pltpu.roll(x, 1, 0))

    def east(x):
        return pltpu.roll(x, nlon - 1, 1)

    def west(x):
        return pltpu.roll(x, 1, 1)

    @pl.loop(0, levs)
    def _(l):
        p, t, q, ec, nc = (r[l] for r in (p_ref, t_ref, q_ref, e_ref, n_ref))
        em = ec * (p + east(p)) * 0.5
        nm = nc * (p + up(p, north_ref[l, 0:1])) * 0.5 * face
        sm = south_ref[l, 3:4] * (south_ref[l, 0:1] + p[0:1]) * 0.5 * face_s
        base = pl.multiple_of(l * 3 * lats, SUB)
        tend[pl.ds(base, lats)] = -((em - west(em)) + (nm - down(nm, sm)) * icc)
        for f, s in ((1, t), (2, q)):
            es = em * (s + east(s)) * 0.5
            ns = nm * (s + up(s, north_ref[l, f : f + 1])) * 0.5
            ss = sm * (south_ref[l, f : f + 1] + s[0:1]) * 0.5
            tend[pl.ds(pl.multiple_of(base + f * lats, SUB), lats)] = -(
                (es - west(es)) + (ns - down(ns, ss)) * icc
            )

    total_rows = tend.shape[0]
    block = 32 if total_rows % 32 == 0 else 16

    @pl.loop(0, total_rows // block)
    def _(rb):
        at = pl.ds(pl.multiple_of(rb * block, 16), block)
        c = [tend[at, a * LANES : (a + 1) * LANES] for a in range(radix)]
        s = [c[a] + c[radix - a] for a in range(1, half + 1)]
        d = [c[a] - c[radix - a] for a in range(1, half + 1)]
        for k1 in range(half + 1):
            re = c[0]
            im = None
            for a in range(1, half + 1):
                angle = 2.0 * math.pi * (a * k1 % radix) / radix
                re = re + s[a - 1] * math.cos(angle)
                if k1:
                    term = d[a - 1] * -math.sin(angle)
                    im = term if im is None else im + term
            lo = 0 if k1 == 0 else LANES + (k1 - 1) * 2 * LANES
            h, w = split_bf16(re)
            yh[at, lo : lo + LANES] = h
            yl[at, lo : lo + LANES] = w
            if k1:
                h, w = split_bf16(im)
                yh[at, lo + LANES : lo + 2 * LANES] = h
                yl[at, lo + LANES : lo + 2 * LANES] = w

    sub_row = lax.broadcasted_iota(jnp.int32, (lats, 2 * LANES), 0)
    cuts = jnp.full((lats, 2 * LANES), nlon, jnp.int32)
    for r in range(lats):
        value = jnp.where(mask_ref[r] > 0, cut_ref[r], nlon)
        cuts = jnp.where(sub_row == r, value, cuts)
    k2 = lax.broadcasted_iota(jnp.int32, (lats, 2 * LANES), 1) % LANES

    dot = functools.partial(jnp.dot, preferred_element_type=jnp.float32)

    def dot_t(a, b):
        return lax.dot_general(a, b, (((1,), (1,)), ((), ())), preferred_element_type=jnp.float32)

    for k1 in range(half + 1):
        lo = 0 if k1 == 0 else LANES + (k1 - 1) * 2 * LANES
        size = LANES if k1 == 0 else 2 * LANES
        mh, ml = mh_ref[k1, :size], ml_ref[k1, :size]
        h, w = yh[:, lo : lo + size], yl[:, lo : lo + size]
        x = dot(h, mh) + dot(h, ml) + dot(w, mh)
        k = k1 + radix * k2
        wave = jnp.minimum(k, nlon - k)
        keep = jnp.where(wave >= cuts, (1.0 if k1 == 0 else 2.0) / nlon, 0.0)
        x = (x.reshape(-1, lats, 2 * LANES) * keep[None]).reshape(-1, 2 * LANES)
        h, w = split_bf16(x)
        spec[:, lo : lo + size] = dot_t(h, mh) + dot_t(h, ml) + dot_t(w, mh)

    part_ref[...] = jnp.zeros_like(part_ref)

    @pl.loop(0, levs)
    def _(l):
        base = pl.multiple_of(l * 3 * lats, SUB)

        def filtered(f):
            at = pl.ds(pl.multiple_of(base + f * lats, SUB), lats)
            z0 = spec[at, 0:LANES]
            re = [spec[at, (2 * k - 1) * LANES : 2 * k * LANES] for k in range(1, half + 1)]
            im = [spec[at, 2 * k * LANES : (2 * k + 1) * LANES] for k in range(1, half + 1)]
            parts = [None] * radix
            for a in range(half + 1):
                even, odd = z0, None
                for k in range(1, half + 1):
                    angle = 2.0 * math.pi * (a * k % radix) / radix
                    even = even + re[k - 1] * math.cos(angle)
                    if a:
                        term = im[k - 1] * math.sin(angle)
                        odd = term if odd is None else odd + term
                if a:
                    parts[a] = even - odd
                    parts[radix - a] = even + odd
                else:
                    parts[0] = even
            return tend[at] - jnp.concatenate(parts, axis=1)

        p, t, q = p_ref[l], t_ref[l], q_ref[l]
        fm = filtered(0)
        np_ = p + fm
        inv = 1.0 / p
        new[pl.ds(base, lats)] = np_
        area = np_ * cc
        acc = part_ref[...]
        for g in range(lats // SUB):
            for a in range(radix):
                acc = acc + area[g * SUB : (g + 1) * SUB, a * LANES : (a + 1) * LANES]
        part_ref[...] = acc
        for f, s in ((1, t), (2, q)):
            new[pl.ds(pl.multiple_of(base + f * lats, SUB), lats)] = s + (filtered(f) - s * fm) * inv

    width = nlon // n_lat
    groups = total_rows // SUB
    full, rest, cap, tail_tiles = pack_plan(width, groups)
    lane = lax.broadcasted_iota(jnp.int32, (SUB, LANES), 1)
    for j in range(n_lat):
        t0, off = divmod(width * j, LANES)
        nt = -(-(off + width) // LANES)
        acc = None
        for g in range(groups):
            x = new[g * SUB : (g + 1) * SUB, t0 * LANES : (t0 + nt) * LANES]
            if off:
                x = pltpu.roll(x, nt * LANES - off, 1)
            for a in range(full):
                send_ref[j, (a * groups + g) * SUB : (a * groups + g + 1) * SUB, :] = x[
                    :, a * LANES : (a + 1) * LANES
                ]
            if rest:
                slot = g % cap
                y = x[:, full * LANES : (full + 1) * LANES]
                if slot:
                    y = pltpu.roll(y, slot * rest, 1)
                acc = y if slot == 0 else jnp.where(lane >= slot * rest, y, acc)
                if slot == cap - 1 or g == groups - 1:
                    o = (full * groups + g // cap) * SUB
                    send_ref[j, o : o + SUB, :] = acc


def exchange_kernel(
    n_lat, n_lev,
    send_ref, part_ref,
    out_ref, sums_ref,
    mid, s1, r1, s2, r2, local, sa, ra, sb, rb,
):
    per = n_lat // n_lev
    i = lax.axis_index("lat")
    l = lax.axis_index("lev")
    owner = i // per
    barrier = pltpu.get_barrier_semaphore()
    for d in range(1, n_lat):
        pl.semaphore_signal(barrier, 1, device_id=((i + d) % n_lat, l), device_id_type=MESH)
    for d in range(1, n_lev):
        pl.semaphore_signal(barrier, 1, device_id=(i, (l + d) % n_lev), device_id_type=MESH)
    pl.semaphore_wait(barrier, n_lat - 1 + n_lev - 1)

    order = sorted(range(1, n_lat), key=lambda d: abs(d - n_lat / 2))

    def remote(src, dst, ss, rs, dev):
        return pltpu.make_async_remote_copy(
            src_ref=src, dst_ref=dst, send_sem=ss, recv_sem=rs, device_id=dev, device_id_type=MESH
        )

    def stage1(d, direct):
        dst = out_ref.at[l * per + i % per] if direct else mid.at[d]
        j = (i + d) % n_lat
        return remote(send_ref.at[j], dst, s1.at[d], r1.at[d], (j, l))

    def sums_a(d):
        j = (i + d) % n_lat
        return remote(part_ref, sums_ref.at[l, i], sa.at[d], ra.at[d], (j, l))

    def sums_b(d):
        return remote(sums_ref.at[l], sums_ref.at[l], sb.at[d], rb.at[d], (i, (l + d) % n_lev))

    own_part = pltpu.make_async_copy(part_ref, sums_ref.at[l, i], local.at[1])
    own_part.start()
    for d in order:
        sums_a(d).start()

    @pl.when(owner == l)
    def _():
        for d in order:
            stage1(d, True).start()
        pltpu.make_async_copy(send_ref.at[i], out_ref.at[l * per + i % per], local.at[0]).start()

    def stage2(d, src_lat, src):
        slot = l * per + src_lat % per
        return remote(src, out_ref.at[slot], s2.at[d], r2.at[slot], (i, src_lat // per))

    @pl.when(owner != l)
    def _():
        for d in order:
            stage1(d, False).start()
        stage2(0, i, send_ref.at[i]).start()

    own_part.wait()
    for d in order:
        sums_a(d).wait_recv()
    for d in range(1, n_lev):
        sums_b(d).start()

    for d in order:
        src_lat = (i + n_lat - d) % n_lat
        stage1(d, False).wait_recv()

        @pl.when(src_lat // per != l)
        def _():
            stage2(d, src_lat, mid.at[d]).start()

    for e in range(1, n_lev):
        for r in range(per):
            slot = ((l + e) % n_lev) * per + r
            remote(mid.at[0], out_ref.at[slot], s2.at[0], r2.at[slot], (i, l)).wait_recv()
    for d in range(1, n_lev):
        sums_b(d).wait_recv()

    for d in order:
        src_lat = (i + n_lat - d) % n_lat
        stage1(d, False).wait_send()
        sums_a(d).wait_send()

        @pl.when(src_lat // per != l)
        def _():
            stage2(d, src_lat, mid.at[d]).wait_send()

    for d in range(1, n_lev):
        sums_b(d).wait_send()

    @pl.when(owner == l)
    def _():
        pltpu.make_async_copy(send_ref.at[i], out_ref.at[l * per + i % per], local.at[0]).wait()

    @pl.when(owner != l)
    def _():
        stage2(0, i, send_ref.at[i]).wait_send()


def remap_kernel(
    n_lat, n_lev, lats, nlon, area_total,
    got_ref, sums_ref, weight_ref, target_ref,
    thick_out, temp_out, tracer_out,
    cols, share, res,
):
    per = n_lat // n_lev
    levels = thick_out.shape[0]
    levs = levels // n_lev
    rgs = lats // SUB
    width = nlon // n_lat
    groups = levs * 3 * rgs
    full, rest, cap, tail_tiles = pack_plan(width, groups)
    lane = lax.broadcasted_iota(jnp.int32, (SUB, LANES), 1)
    outs = (thick_out, temp_out, tracer_out)

    whole = jnp.full((SUB, LANES), weight_ref[0])
    for k in range(1, levels):
        whole = whole + weight_ref[k]
    run = jnp.zeros((SUB, LANES), jnp.float32)
    for k in range(levels):
        part = jnp.full((SUB, LANES), weight_ref[k]) / whole
        run = run + part
        share[0, k] = part
        share[1, k] = run
        share[2, k] = 1.0 / part
    sums = sums_ref[...].reshape(-1, SUB, LANES)
    total = jnp.sum(jnp.sum(sums, axis=0), keepdims=True)
    factor = jnp.full((1, 1), target_ref[0] * (nlon * area_total)) / total

    n_main = full * per * rgs
    col_groups = per * rgs
    for lev in range(n_lev):
        for ll in range(levs):
            for f in range(3):
                acc = None
                for rs in range(per):
                    for rg in range(rgs):
                        g = (ll * 3 + f) * rgs + rg
                        for a in range(full):
                            v = (a * per + rs) * rgs + rg
                            o = (a * groups + g) * SUB
                            cols[f, lev * levs + ll, v] = got_ref[lev * per + rs, o : o + SUB, :]
                        if rest:
                            o = (full * groups + g // cap) * SUB
                            y = got_ref[lev * per + rs, o : o + SUB, :]
                            cg = rs * rgs + rg
                            slot = cg % cap
                            shift = (slot - g % cap) * rest % LANES
                            if shift:
                                y = pltpu.roll(y, shift, 1)
                            acc = (
                                y if slot == 0
                                else jnp.where(lane >= slot * rest, y, acc)
                            )
                            if slot == cap - 1 or cg == col_groups - 1:
                                last = (slot + 1) * rest
                                if last < LANES:
                                    acc = jnp.where(lane < last, acc, 1.0)
                                cols[f, lev * levs + ll, n_main + cg // cap] = acc

    def remap(v, put):
        thick = [cols[0, m, v] for m in range(levels)]
        tops = []
        surface = jnp.zeros((SUB, LANES), jnp.float32)
        for m in range(levels):
            tops.append(surface)
            surface = surface + thick[m]
        inv = 1.0 / surface
        scale = surface * factor
        before = (jnp.zeros_like(surface), jnp.zeros_like(surface))
        for k in range(levels):
            bound = surface * share[1, k]
            ct = cq = None
            for m in range(levels):
                w = jnp.minimum(jnp.maximum(bound - tops[m], 0.0), thick[m])
                dt, dq = cols[1, m, v] * w, cols[2, m, v] * w
                ct, cq = (dt, dq) if m == 0 else (ct + dt, cq + dq)
            per_share = inv * share[2, k]
            put(k, scale * share[0, k], (ct - before[0]) * per_share, (cq - before[1]) * per_share)
            before = (ct, cq)

    if full:
        for a in range(full):
            @pl.loop(0, col_groups)
            def _(v):
                at = pl.ds(pl.multiple_of(v * SUB, SUB), SUB)

                def put(k, *values):
                    for ref, x in zip(outs, values):
                        ref[k, at, a * LANES : (a + 1) * LANES] = x

                remap(a * col_groups + v, put)

    if rest:
        n_tail = -(-col_groups // cap)

        @pl.loop(0, n_tail)
        def _(v):
            def put(k, *values):
                for f, x in enumerate(values):
                    res[f, k, v] = x

            remap(n_main + v, put)

        for cg in range(col_groups):
            @pl.loop(0, levels)
            def _(k):
                for f in range(3):
                    x = res[f, k, cg // cap]
                    if cg % cap:
                        x = pltpu.roll(x, LANES - (cg % cap) * rest, 1)
                    outs[f][k, cg * SUB : (cg + 1) * SUB, full * LANES : full * LANES + rest] = x[:, :rest]


def on_device(p, t, q, ec, nc, polar_mask, wave_cutoff, level_weight, target_surface):
    levs, lats, nlon = p.shape
    n_lat, n_lev = lax.axis_size("lat"), lax.axis_size("lev")
    nlat = lats * n_lat
    levels = levs * n_lev
    per = n_lat // n_lev
    width = nlon // n_lat
    f32 = jnp.float32
    tail = jnp.stack([p[:, -1], t[:, -1], q[:, -1], nc[:, -1]], axis=1)
    head = jnp.stack([p[:, 0], t[:, 0], q[:, 0]], axis=1)
    south = lax.ppermute(tail, "lat", [(i, i + 1) for i in range(n_lat - 1)])
    north = lax.ppermute(head, "lat", [(i + 1, i) for i in range(n_lat - 1)])
    high, low = dft_tables(nlon)
    rows = levs * 3 * lats
    groups = rows // SUB
    full, rest, cap, tail_tiles = pack_plan(width, groups)
    packed = (full * groups + tail_tiles) * SUB
    limit = pltpu.CompilerParams(vmem_limit_bytes=48 * 1024 * 1024)
    send, part = pl.pallas_call(
        functools.partial(update_kernel, n_lat),
        out_shape=(
            jax.ShapeDtypeStruct((n_lat, packed, LANES), f32),
            jax.ShapeDtypeStruct((SUB, LANES), f32),
        ),
        in_specs=[VMEM] * 7 + [SMEM] * 2 + [VMEM] * 3,
        out_specs=(VMEM, VMEM),
        scratch_shapes=[
            pltpu.VMEM((rows, nlon), f32),
            pltpu.VMEM((rows, nlon), f32),
            pltpu.VMEM((rows, nlon), f32),
            pltpu.VMEM((rows, nlon), jnp.bfloat16),
            pltpu.VMEM((rows, nlon), jnp.bfloat16),
        ],
        compiler_params=limit,
        name="update",
    )(p, t, q, ec, nc, south, north, polar_mask, wave_cutoff, jnp.asarray(row_tables(nlat)),
      jnp.asarray(high), jnp.asarray(low))

    dma = pltpu.SemaphoreType.DMA
    got, sums = pl.pallas_call(
        functools.partial(exchange_kernel, n_lat, n_lev),
        out_shape=(
            jax.ShapeDtypeStruct((n_lev * per, packed, LANES), f32),
            jax.ShapeDtypeStruct((n_lev, n_lat, SUB, LANES), f32),
        ),
        in_specs=[VMEM, VMEM],
        out_specs=(VMEM, VMEM),
        scratch_shapes=[
            pltpu.VMEM((n_lat, packed, LANES), f32),
            dma((n_lat,)), dma((n_lat,)), dma((n_lat,)), dma((n_lev * per,)), dma((2,)),
            dma((n_lat,)), dma((n_lat,)), dma((n_lev,)), dma((n_lev,)),
        ],
        compiler_params=pltpu.CompilerParams(
            collective_id=0, has_side_effects=True, vmem_limit_bytes=32 * 1024 * 1024
        ),
        name="exchange",
    )(send, part)

    area_total = float(np.sum(np.sin((np.arange(nlat) + 0.5) * np.pi / nlat)))
    col_groups = per * lats // SUB
    n_tail = -(-col_groups // cap) if rest else 0
    out = jax.ShapeDtypeStruct((levels, nlat // n_lev, width), f32)
    return pl.pallas_call(
        functools.partial(remap_kernel, n_lat, n_lev, lats, nlon, area_total),
        out_shape=(out, out, out),
        in_specs=[VMEM, VMEM, SMEM, SMEM],
        out_specs=(VMEM, VMEM, VMEM),
        scratch_shapes=[
            pltpu.VMEM((3, levels, full * col_groups + n_tail, SUB, LANES), f32),
            pltpu.VMEM((3, levels, SUB, LANES), f32),
            pltpu.VMEM((3, levels, max(n_tail, 1), SUB, LANES), f32),
        ],
        compiler_params=limit,
        name="remap",
    )(got, sums, level_weight, target_surface)


def solution(mesh):
    return jax.shard_map(
        on_device,
        mesh=mesh,
        in_specs=(P("lev", "lat", None),) * 5 + (P("lat"), P("lat"), P(), P()),
        out_specs=(P(None, "lev", "lat"),) * 3,
        check_vma=False,
    )
```

```python
import functools
import math

import jax
import jax.numpy as jnp
import numpy as np
from jax import lax
from jax.experimental import pallas as pl
from jax.experimental.pallas import tpu as pltpu
from jax.sharding import PartitionSpec as P

LANES = 128
SUB = 8
VMEM = pl.BlockSpec(memory_space=pltpu.VMEM)
SMEM = pl.BlockSpec(memory_space=pltpu.SMEM)
MESH = pl.DeviceIdType.MESH


@functools.cache
def dft_tables(nlon):
    radix = nlon // LANES
    b = np.arange(LANES)[:, None]
    k2 = np.arange(LANES)[None, :]
    high, low = [], []
    for k1 in range(radix // 2 + 1):
        phase = (b * (k1 + radix * k2) % nlon) * (2.0 * np.pi / nlon)
        c, s = np.cos(phase), np.sin(phase)
        table = np.block([[c, -s], [s, c]]).astype(np.float32)
        top = table.astype(jnp.bfloat16)
        high.append(top)
        low.append((table - top.astype(np.float32)).astype(jnp.bfloat16))
    return np.stack(high), np.stack(low)


@functools.cache
def row_tables(nlat):
    rows = np.arange(nlat, dtype=np.float64)
    out = np.zeros((nlat, LANES), np.float32)
    out[:, 0] = np.sin((rows + 0.5) * np.pi / nlat)
    out[:, 1] = 1.0 / np.sin((rows + 0.5) * np.pi / nlat)
    out[:, 2] = np.sin((rows + 1.0) * np.pi / nlat)
    out[:, 3] = np.sin(rows * np.pi / nlat)
    return out


def pack_plan(width, groups):
    full, rest = divmod(width, LANES)
    cap = LANES // rest if rest else 1
    tail_tiles = -(-groups // cap) if rest else 0
    return full, rest, cap, tail_tiles


def split_bf16(x):
    top = x.astype(jnp.bfloat16)
    return top, (x - top.astype(jnp.float32)).astype(jnp.bfloat16)


def step_kernel(
    n_lat, n_lev, chunks,
    p_hbm, t_hbm, q_hbm, e_hbm, n_hbm, rows_hbm, mh_hbm, ml_hbm, mask_ref, cut_ref,
    out_ref, sums_ref,
    p_ref, t_ref, q_ref, e_ref, n_ref, rows_ref, mh_ref, ml_ref,
    last, head_rows, tail, head, south_ref, north_ref, tend, spec, new, yh, yl,
    send_ref, part_ref, mid,
    ins, edge, send_sem, recv_sem, s1, r1, s2, r2, local, sa, ra, sb, rb,
):
    levs, lats, nlon = p_hbm.shape
    i = lax.axis_index("lat")
    l = lax.axis_index("lev")
    barrier = pltpu.get_barrier_semaphore()

    for d in range(1, n_lat):
        pl.semaphore_signal(barrier, 1, device_id=((i + d) % n_lat, l), device_id_type=MESH)
    for d in range(1, n_lev):
        pl.semaphore_signal(barrier, 1, device_id=(i, (l + d) % n_lev), device_id_type=MESH)

    edges = []
    for f, ref in enumerate((p_hbm, t_hbm, q_hbm, n_hbm)):
        edges.append(pltpu.make_async_copy(ref.at[:, lats - SUB :, :], last.at[f], edge.at[0, f]))
    for f, ref in enumerate((p_hbm, t_hbm, q_hbm)):
        edges.append(pltpu.make_async_copy(ref.at[:, :SUB, :], head_rows.at[f], edge.at[1, f]))
    for copy in edges:
        copy.start()
    pairs = (
        (p_hbm, p_ref), (t_hbm, t_ref), (q_hbm, q_ref), (e_hbm, e_ref), (n_hbm, n_ref),
        (rows_hbm, rows_ref), (mh_hbm, mh_ref), (ml_hbm, ml_ref),
    )
    loads = [pltpu.make_async_copy(a, b, ins.at[c]) for c, (a, b) in enumerate(pairs)]
    for copy in loads:
        copy.start()
    for copy in edges:
        copy.wait()
    for f in range(4):
        for lev in range(levs):
            tail[lev, f : f + 1, :] = last[f, lev, SUB - 1 : SUB, :]
    for f in range(3):
        for lev in range(levs):
            head[lev, f : f + 1, :] = head_rows[f, lev, 0:1, :]
    for lev in range(levs):
        head[lev, 3:4, :] = jnp.zeros((1, nlon), jnp.float32)

    def send(src, dst, c, to):
        return pltpu.make_async_remote_copy(
            src_ref=src, dst_ref=dst, send_sem=send_sem.at[c], recv_sem=recv_sem.at[c],
            device_id=(to, l), device_id_type=MESH,
        )

    pl.semaphore_wait(barrier, n_lat - 1 + n_lev - 1)

    @pl.when(i < n_lat - 1)
    def _():
        send(tail, south_ref, 0, i + 1).start()

    @pl.when(i > 0)
    def _():
        send(head, north_ref, 1, i - 1).start()

    @pl.when(i == 0)
    def _():
        south_ref[...] = jnp.zeros_like(south_ref)

    @pl.when(i == n_lat - 1)
    def _():
        north_ref[...] = jnp.zeros_like(north_ref)

    for copy in loads:
        copy.wait()

    @pl.when(i < n_lat - 1)
    def _():
        send(tail, south_ref, 0, i + 1).wait_send()
        send(head, north_ref, 1, i + 1).wait_recv()

    @pl.when(i > 0)
    def _():
        send(head, north_ref, 1, i - 1).wait_send()
        send(tail, south_ref, 0, i - 1).wait_recv()

    order = sorted(range(1, n_lat), key=lambda d: abs(d - n_lat / 2))
    per = n_lat // n_lev
    owner = i // per
    own_slot = l * per + i % per

    def remote(src, dst, ss, rs, dev):
        return pltpu.make_async_remote_copy(
            src_ref=src, dst_ref=dst, send_sem=ss, recv_sem=rs, device_id=dev, device_id_type=MESH
        )

    def stage1(d, c, direct):
        dst = out_ref.at[own_slot, c] if direct else mid.at[d, c]
        j = (i + d) % n_lat
        return remote(send_ref.at[j, c], dst, s1.at[d, c], r1.at[d, c], (j, l))

    def stage2(d, c, src_lat, src):
        slot = l * per + src_lat % per
        return remote(src, out_ref.at[slot, c], s2.at[d, c], r2.at[slot, c], (i, src_lat // per))

    def own_block(c):
        return pltpu.make_async_copy(send_ref.at[i, c], out_ref.at[own_slot, c], local.at[c])

    def sums_a(d):
        j = (i + d) % n_lat
        return remote(part_ref, sums_ref.at[l, i], sa.at[d], ra.at[d], (j, l))

    def sums_b(d):
        return remote(sums_ref.at[l], sums_ref.at[l], sb.at[d], rb.at[d], (i, (l + d) % n_lev))

    radix = nlon // LANES
    half = radix // 2
    first = pl.multiple_of(lax.axis_index("lat") * lats, SUB)
    table = rows_ref[pl.ds(first, lats), :]
    cc, icc, face, face_s = (table[:, c : c + 1] for c in range(4))
    face_s = face_s[0:1]
    row = lax.broadcasted_iota(jnp.int32, (lats, nlon), 0)

    def up(x, halo):
        return jnp.where(row == lats - 1, halo, pltpu.roll(x, lats - 1, 0))

    def down(x, halo):
        return jnp.where(row == 0, halo, pltpu.roll(x, 1, 0))

    def east(x):
        return pltpu.roll(x, nlon - 1, 1)

    def west(x):
        return pltpu.roll(x, 1, 1)

    clevs = levs // chunks
    sub_row = lax.broadcasted_iota(jnp.int32, (lats, 2 * LANES), 0)
    cuts = jnp.full((lats, 2 * LANES), nlon, jnp.int32)
    for r in range(lats):
        value = jnp.where(mask_ref[r] > 0, cut_ref[r], nlon)
        cuts = jnp.where(sub_row == r, value, cuts)
    k2 = lax.broadcasted_iota(jnp.int32, (lats, 2 * LANES), 1) % LANES

    dot = functools.partial(jnp.dot, preferred_element_type=jnp.float32)

    def dot_t(a, b):
        return lax.dot_general(a, b, (((1,), (1,)), ((), ())), preferred_element_type=jnp.float32)

    part_ref[...] = jnp.zeros_like(part_ref)

    for chunk in range(chunks):
        @pl.loop(0, clevs)
        def _(cl):
            l = cl + chunk * clevs
            p, t, q, ec, nc = (r[l] for r in (p_ref, t_ref, q_ref, e_ref, n_ref))
            em = ec * (p + east(p)) * 0.5
            nm = nc * (p + up(p, north_ref[l, 0:1])) * 0.5 * face
            sm = south_ref[l, 3:4] * (south_ref[l, 0:1] + p[0:1]) * 0.5 * face_s
            base = pl.multiple_of(cl * 3 * lats, SUB)
            tend[pl.ds(base, lats)] = -((em - west(em)) + (nm - down(nm, sm)) * icc)
            for f, s in ((1, t), (2, q)):
                es = em * (s + east(s)) * 0.5
                ns = nm * (s + up(s, north_ref[l, f : f + 1])) * 0.5
                ss = sm * (south_ref[l, f : f + 1] + s[0:1]) * 0.5
                tend[pl.ds(pl.multiple_of(base + f * lats, SUB), lats)] = -(
                    (es - west(es)) + (ns - down(ns, ss)) * icc
                )

        total_rows = tend.shape[0]
        block = 48 if total_rows % 48 == 0 else 16

        @pl.loop(0, total_rows // block)
        def _(rb):
            at = pl.ds(pl.multiple_of(rb * block, 16), block)
            c = [tend[at, a * LANES : (a + 1) * LANES] for a in range(radix)]
            s = [c[a] + c[radix - a] for a in range(1, half + 1)]
            d = [c[a] - c[radix - a] for a in range(1, half + 1)]
            for k1 in range(half + 1):
                re = c[0]
                im = None
                for a in range(1, half + 1):
                    angle = 2.0 * math.pi * (a * k1 % radix) / radix
                    re = re + s[a - 1] * math.cos(angle)
                    if k1:
                        term = d[a - 1] * -math.sin(angle)
                        im = term if im is None else im + term
                lo = 0 if k1 == 0 else LANES + (k1 - 1) * 2 * LANES
                h, w = split_bf16(re)
                yh[at, lo : lo + LANES] = h
                yl[at, lo : lo + LANES] = w
                if k1:
                    h, w = split_bf16(im)
                    yh[at, lo + LANES : lo + 2 * LANES] = h
                    yl[at, lo + LANES : lo + 2 * LANES] = w

        for k1 in range(half + 1):
            lo = 0 if k1 == 0 else LANES + (k1 - 1) * 2 * LANES
            size = LANES if k1 == 0 else 2 * LANES
            mh, ml = mh_ref[k1, :size], ml_ref[k1, :size]
            h, w = yh[:, lo : lo + size], yl[:, lo : lo + size]
            x = dot(h, mh) + dot(h, ml) + dot(w, mh)
            k = k1 + radix * k2
            wave = jnp.minimum(k, nlon - k)
            keep = jnp.where(wave >= cuts, (1.0 if k1 == 0 else 2.0) / nlon, 0.0)
            x = (x.reshape(-1, lats, 2 * LANES) * keep[None]).reshape(-1, 2 * LANES)
            h, w = split_bf16(x)
            spec[:, lo : lo + size] = dot_t(h, mh) + dot_t(h, ml) + dot_t(w, mh)

        @pl.loop(0, clevs)
        def _(cl):
            l = cl + chunk * clevs
            base = pl.multiple_of(cl * 3 * lats, SUB)

            def filtered(f):
                at = pl.ds(pl.multiple_of(base + f * lats, SUB), lats)
                z0 = spec[at, 0:LANES]
                re = [spec[at, (2 * k - 1) * LANES : 2 * k * LANES] for k in range(1, half + 1)]
                im = [spec[at, 2 * k * LANES : (2 * k + 1) * LANES] for k in range(1, half + 1)]
                parts = [None] * radix
                for a in range(half + 1):
                    even, odd = z0, None
                    for k in range(1, half + 1):
                        angle = 2.0 * math.pi * (a * k % radix) / radix
                        even = even + re[k - 1] * math.cos(angle)
                        if a:
                            term = im[k - 1] * math.sin(angle)
                            odd = term if odd is None else odd + term
                    if a:
                        parts[a] = even - odd
                        parts[radix - a] = even + odd
                    else:
                        parts[0] = even
                return tend[at] - jnp.concatenate(parts, axis=1)

            p, t, q = p_ref[l], t_ref[l], q_ref[l]
            fm = filtered(0)
            np_ = p + fm
            inv = 1.0 / p
            new[pl.ds(base, lats)] = np_
            area = np_ * cc
            acc = part_ref[...]
            for g in range(lats // SUB):
                for a in range(radix):
                    acc = acc + area[g * SUB : (g + 1) * SUB, a * LANES : (a + 1) * LANES]
            part_ref[...] = acc
            for f, s in ((1, t), (2, q)):
                new[pl.ds(pl.multiple_of(base + f * lats, SUB), lats)] = s + (filtered(f) - s * fm) * inv

        width = nlon // n_lat
        groups = total_rows // SUB
        full, rest, cap, tail_tiles = pack_plan(width, groups)
        lane = lax.broadcasted_iota(jnp.int32, (SUB, LANES), 1)
        for j in range(n_lat):
            t0, off = divmod(width * j, LANES)
            nt = -(-(off + width) // LANES)
            acc = None
            for g in range(groups):
                x = new[g * SUB : (g + 1) * SUB, t0 * LANES : (t0 + nt) * LANES]
                if off:
                    x = pltpu.roll(x, nt * LANES - off, 1)
                for a in range(full):
                    send_ref[j, chunk, (a * groups + g) * SUB : (a * groups + g + 1) * SUB, :] = x[
                        :, a * LANES : (a + 1) * LANES
                    ]
                if rest:
                    slot = g % cap
                    y = x[:, full * LANES : (full + 1) * LANES]
                    if slot:
                        y = pltpu.roll(y, slot * rest, 1)
                    acc = y if slot == 0 else jnp.where(lane >= slot * rest, y, acc)
                    if slot == cap - 1 or g == groups - 1:
                        o = (full * groups + g // cap) * SUB
                        send_ref[j, chunk, o : o + SUB, :] = acc


        @pl.when(owner == l)
        def _():
            for d in order:
                stage1(d, chunk, True).start()
            own_block(chunk).start()

        @pl.when(owner != l)
        def _():
            for d in order:
                stage1(d, chunk, False).start()
            stage2(0, chunk, i, send_ref.at[i, chunk]).start()


    own_part = pltpu.make_async_copy(part_ref, sums_ref.at[l, i], local.at[chunks])
    own_part.start()
    for d in order:
        sums_a(d).start()
    for c in range(chunks):
        for d in order:
            src_lat = (i + n_lat - d) % n_lat
            stage1(d, c, False).wait_recv()

            @pl.when(src_lat // per != l)
            def _():
                stage2(d, c, src_lat, mid.at[d, c]).start()

        if c == 0:
            own_part.wait()
            for d in order:
                sums_a(d).wait_recv()
            for d in range(1, n_lev):
                sums_b(d).start()

    for e in range(1, n_lev):
        for r in range(per):
            slot = ((l + e) % n_lev) * per + r
            for c in range(chunks):
                remote(mid.at[0, c], out_ref.at[slot, c], s2.at[0, c], r2.at[slot, c], (i, l)).wait_recv()
    for d in range(1, n_lev):
        sums_b(d).wait_recv()

    for d in order:
        sums_a(d).wait_send()
        src_lat = (i + n_lat - d) % n_lat
        for c in range(chunks):
            stage1(d, c, False).wait_send()

        @pl.when(src_lat // per != l)
        def _():
            for c in range(chunks):
                stage2(d, c, src_lat, mid.at[d, c]).wait_send()

    for d in range(1, n_lev):
        sums_b(d).wait_send()

    @pl.when(owner == l)
    def _():
        for c in range(chunks):
            own_block(c).wait()

    @pl.when(owner != l)
    def _():
        for c in range(chunks):
            stage2(0, c, i, send_ref.at[i, c]).wait_send()


def remap_kernel(
    n_lat, n_lev, chunks, lats, nlon, area_total,
    got_hbm, sums_ref, weight_ref, target_ref,
    thick_out, temp_out, tracer_out,
    cols, share, res, got, thick_buf, temp_buf, tracer_buf, in_sem, out_sem,
):
    per = n_lat // n_lev
    levels = thick_out.shape[0]
    levs = levels // n_lev
    rgs = lats // SUB
    width = nlon // n_lat
    clevs = levs // chunks
    groups = clevs * 3 * rgs
    full, rest, cap, tail_tiles = pack_plan(width, groups)
    lane = lax.broadcasted_iota(jnp.int32, (SUB, LANES), 1)
    outs = (thick_buf, temp_buf, tracer_buf)
    finals = (thick_out, temp_out, tracer_out)
    loads = [
        pltpu.make_async_copy(got_hbm.at[slot], got.at[slot], in_sem.at[slot])
        for slot in range(n_lev * per)
    ]
    for copy in loads:
        copy.start()

    whole = jnp.full((SUB, LANES), weight_ref[0])
    for k in range(1, levels):
        whole = whole + weight_ref[k]
    run = jnp.zeros((SUB, LANES), jnp.float32)
    for k in range(levels):
        part = jnp.full((SUB, LANES), weight_ref[k]) / whole
        run = run + part
        share[0, k] = part
        share[1, k] = run
        share[2, k] = 1.0 / part
    sums = sums_ref[...].reshape(-1, SUB, LANES)
    total = jnp.sum(jnp.sum(sums, axis=0), keepdims=True)
    factor = jnp.full((1, 1), target_ref[0] * (nlon * area_total)) / total

    n_main = full * per * rgs
    col_groups = per * rgs
    for lev in range(n_lev):
        for rs in range(per):
            loads[lev * per + rs].wait()
        for ll in range(levs):
            c, cl = divmod(ll, clevs)
            for f in range(3):
                acc = None
                for rs in range(per):
                    for rg in range(rgs):
                        g = (cl * 3 + f) * rgs + rg
                        for a in range(full):
                            v = (a * per + rs) * rgs + rg
                            o = (a * groups + g) * SUB
                            cols[f, lev * levs + ll, v] = got[lev * per + rs, c, o : o + SUB, :]
                        if rest:
                            o = (full * groups + g // cap) * SUB
                            y = got[lev * per + rs, c, o : o + SUB, :]
                            cg = rs * rgs + rg
                            slot = cg % cap
                            shift = (slot - g % cap) * rest % LANES
                            if shift:
                                y = pltpu.roll(y, shift, 1)
                            acc = (
                                y if slot == 0
                                else jnp.where(lane >= slot * rest, y, acc)
                            )
                            if slot == cap - 1 or cg == col_groups - 1:
                                last = (slot + 1) * rest
                                if last < LANES:
                                    acc = jnp.where(lane < last, acc, 1.0)
                                cols[f, lev * levs + ll, n_main + cg // cap] = acc

    def remap(v, put):
        thick = [cols[0, m, v] for m in range(levels)]
        tops = []
        surface = jnp.zeros((SUB, LANES), jnp.float32)
        for m in range(levels):
            tops.append(surface)
            surface = surface + thick[m]
        inv = 1.0 / surface
        scale = surface * factor
        before = (jnp.zeros_like(surface), jnp.zeros_like(surface))
        for k in range(levels):
            bound = surface * share[1, k]
            ct = cq = None
            for m in range(levels):
                w = jnp.minimum(jnp.maximum(bound - tops[m], 0.0), thick[m])
                dt, dq = cols[1, m, v] * w, cols[2, m, v] * w
                ct, cq = (dt, dq) if m == 0 else (ct + dt, cq + dq)
            per_share = inv * share[2, k]
            put(k, scale * share[0, k], (ct - before[0]) * per_share, (cq - before[1]) * per_share)
            before = (ct, cq)

    if rest:
        n_tail = -(-col_groups // cap)

        @pl.loop(0, n_tail)
        def _(v):
            def put(k, *values):
                for f, x in enumerate(values):
                    res[f, k, v] = x

            remap(n_main + v, put)

        for cg in range(col_groups):
            @pl.loop(0, levels)
            def _(k):
                for f in range(3):
                    x = res[f, k, cg // cap]
                    if cg % cap:
                        x = pltpu.roll(x, LANES - (cg % cap) * rest, 1)
                    outs[f][k, cg * SUB : (cg + 1) * SUB, full * LANES : full * LANES + rest] = x[:, :rest]

    def finish(v):
        at = pl.ds(pl.multiple_of(v * SUB, SUB), SUB)
        return [
            pltpu.make_async_copy(outs[f].at[:, at, :], finals[f].at[:, at, :], out_sem.at[f, v])
            for f in range(3)
        ]

    for a in range(full):
        @pl.loop(0, col_groups)
        def _(v):
            at = pl.ds(pl.multiple_of(v * SUB, SUB), SUB)

            def put(k, *values):
                for ref, x in zip(outs, values):
                    ref[k, at, a * LANES : (a + 1) * LANES] = x

            remap(a * col_groups + v, put)
            if a == full - 1:
                for copy in finish(v):
                    copy.start()

    if not full:
        for v in range(col_groups):
            for copy in finish(v):
                copy.start()
    for v in range(col_groups):
        for copy in finish(v):
            copy.wait()


def on_device(p, t, q, ec, nc, polar_mask, wave_cutoff, level_weight, target_surface):
    levs, lats, nlon = p.shape
    n_lat, n_lev = lax.axis_size("lat"), lax.axis_size("lev")
    nlat = lats * n_lat
    levels = levs * n_lev
    per = n_lat // n_lev
    width = nlon // n_lat
    f32 = jnp.float32
    high, low = dft_tables(nlon)
    chunks = 2
    rows = levs * 3 * lats
    crows = rows // chunks
    groups = crows // SUB
    full, rest, cap, tail_tiles = pack_plan(width, groups)
    packed = (full * groups + tail_tiles) * SUB
    dma = pltpu.SemaphoreType.DMA
    grant = 62_800_000
    given = (p, t, q, ec, nc, jnp.asarray(row_tables(nlat)), jnp.asarray(high), jnp.asarray(low))
    hbm = pl.BlockSpec(memory_space=pltpu.HBM)
    got, sums = pl.pallas_call(
        functools.partial(step_kernel, n_lat, n_lev, chunks),
        out_shape=(
            jax.ShapeDtypeStruct((n_lat, chunks, packed, LANES), f32),
            jax.ShapeDtypeStruct((n_lev, n_lat, SUB, LANES), f32),
        ),
        in_specs=[hbm] * 8 + [SMEM] * 2,
        out_specs=(hbm, hbm),
        scratch_shapes=[pltpu.VMEM(x.shape, x.dtype) for x in given] + [
            pltpu.VMEM((4, levs, SUB, nlon), f32),
            pltpu.VMEM((3, levs, SUB, nlon), f32),
            pltpu.VMEM((levs, 4, nlon), f32),
            pltpu.VMEM((levs, 4, nlon), f32),
            pltpu.VMEM((levs, 4, nlon), f32),
            pltpu.VMEM((levs, 4, nlon), f32),
            pltpu.VMEM((crows, nlon), f32),
            pltpu.VMEM((crows, nlon), f32),
            pltpu.VMEM((crows, nlon), f32),
            pltpu.VMEM((crows, nlon), jnp.bfloat16),
            pltpu.VMEM((crows, nlon), jnp.bfloat16),
            pltpu.VMEM((n_lat, chunks, packed, LANES), f32),
            pltpu.VMEM((SUB, LANES), f32),
            pltpu.VMEM((n_lat, chunks, packed, LANES), f32),
            dma((8,)), dma((2, 4)), dma((2,)), dma((2,)),
            dma((n_lat, chunks)), dma((n_lat, chunks)), dma((n_lat, chunks)), dma((n_lat, chunks)),
            dma((chunks + 1,)), dma((n_lat,)), dma((n_lat,)), dma((n_lev,)), dma((n_lev,)),
        ],
        compiler_params=pltpu.CompilerParams(
            collective_id=0, has_side_effects=True, vmem_limit_bytes=grant
        ),
        name="step",
    )(*given, polar_mask, wave_cutoff)

    area_total = float(np.sum(np.sin((np.arange(nlat) + 0.5) * np.pi / nlat)))
    col_groups = per * lats // SUB
    n_tail = -(-col_groups // cap) if rest else 0
    out = jax.ShapeDtypeStruct((levels, nlat // n_lev, width), f32)
    return pl.pallas_call(
        functools.partial(remap_kernel, n_lat, n_lev, chunks, lats, nlon, area_total),
        out_shape=(out, out, out),
        in_specs=[hbm, VMEM, SMEM, SMEM],
        out_specs=(hbm, hbm, hbm),
        scratch_shapes=[
            pltpu.VMEM((3, levels, full * col_groups + n_tail, SUB, LANES), f32),
            pltpu.VMEM((3, levels, SUB, LANES), f32),
            pltpu.VMEM((3, levels, max(n_tail, 1), SUB, LANES), f32),
            pltpu.VMEM(got.shape, f32),
            pltpu.VMEM(out.shape, f32), pltpu.VMEM(out.shape, f32), pltpu.VMEM(out.shape, f32),
            dma((n_lat,)), dma((3, col_groups)),
        ],
        compiler_params=pltpu.CompilerParams(vmem_limit_bytes=grant),
        name="remap",
    )(got, sums, level_weight, target_surface)


def solution(mesh):
    return jax.shard_map(
        on_device,
        mesh=mesh,
        in_specs=(P("lev", "lat", None),) * 5 + (P("lat"), P("lat"), P(), P()),
        out_specs=(P(None, "lev", "lat"),) * 3,
        check_vma=False,
    )
```

```python
import functools
import math

import jax
import jax.numpy as jnp
import numpy as np
from jax import lax
from jax.experimental import pallas as pl
from jax.experimental.pallas import tpu as pltpu
from jax.sharding import PartitionSpec as P

LANES = 128
SUB = 8
VMEM = pl.BlockSpec(memory_space=pltpu.VMEM)
SMEM = pl.BlockSpec(memory_space=pltpu.SMEM)
MESH = pl.DeviceIdType.MESH


@functools.cache
def dft_tables(nlon):
    radix = nlon // LANES
    b = np.arange(LANES)[:, None]
    k2 = np.arange(LANES)[None, :]
    high, low = [], []
    for k1 in range(radix // 2 + 1):
        phase = (b * (k1 + radix * k2) % nlon) * (2.0 * np.pi / nlon)
        c, s = np.cos(phase), np.sin(phase)
        table = np.block([[c, -s], [s, c]]).astype(np.float32)
        top = table.astype(jnp.bfloat16)
        high.append(top)
        low.append((table - top.astype(np.float32)).astype(jnp.bfloat16))
    return np.stack(high), np.stack(low)


@functools.cache
def row_tables(nlat):
    rows = np.arange(nlat, dtype=np.float64)
    out = np.zeros((nlat, LANES), np.float32)
    out[:, 0] = np.sin((rows + 0.5) * np.pi / nlat)
    out[:, 1] = 1.0 / np.sin((rows + 0.5) * np.pi / nlat)
    out[:, 2] = np.sin((rows + 1.0) * np.pi / nlat)
    out[:, 3] = np.sin(rows * np.pi / nlat)
    return out


def pack_plan(width, groups):
    full, rest = divmod(width, LANES)
    cap = LANES // rest if rest else 1
    tail_tiles = -(-groups // cap) if rest else 0
    return full, rest, cap, tail_tiles


def split_bf16(x):
    top = x.astype(jnp.bfloat16)
    return top, (x - top.astype(jnp.float32)).astype(jnp.bfloat16)


def step_kernel(
    n_lat, n_lev, chunks,
    p_hbm, t_hbm, q_hbm, e_hbm, n_hbm, rows_hbm, mh_hbm, ml_hbm, mask_ref, cut_ref,
    out_ref, sums_ref,
    p_ref, t_ref, q_ref, e_ref, n_ref, rows_ref, mh_ref, ml_ref,
    last, head_rows, tail, head, south_ref, north_ref, tend, spec, new, yh, yl,
    send_ref, part_ref, mid,
    ins, edge, send_sem, recv_sem, s1, r1, s2, r2, local, sa, ra, sb, rb,
):
    levs, lats, nlon = p_hbm.shape
    i = lax.axis_index("lat")
    l = lax.axis_index("lev")
    barrier = pltpu.get_barrier_semaphore()

    for d in range(1, n_lat):
        pl.semaphore_signal(barrier, 1, device_id=((i + d) % n_lat, l), device_id_type=MESH)
    for d in range(1, n_lev):
        pl.semaphore_signal(barrier, 1, device_id=(i, (l + d) % n_lev), device_id_type=MESH)

    edges = []
    for f, ref in enumerate((p_hbm, t_hbm, q_hbm, n_hbm)):
        edges.append(pltpu.make_async_copy(ref.at[:, lats - SUB :, :], last.at[f], edge.at[0, f]))
    for f, ref in enumerate((p_hbm, t_hbm, q_hbm)):
        edges.append(pltpu.make_async_copy(ref.at[:, :SUB, :], head_rows.at[f], edge.at[1, f]))
    for copy in edges:
        copy.start()
    pairs = (
        (p_hbm, p_ref), (t_hbm, t_ref), (q_hbm, q_ref), (e_hbm, e_ref), (n_hbm, n_ref),
        (rows_hbm, rows_ref), (mh_hbm, mh_ref), (ml_hbm, ml_ref),
    )
    loads = [pltpu.make_async_copy(a, b, ins.at[c]) for c, (a, b) in enumerate(pairs)]
    for copy in loads:
        copy.start()
    for copy in edges:
        copy.wait()
    for f in range(4):
        for lev in range(levs):
            tail[lev, f : f + 1, :] = last[f, lev, SUB - 1 : SUB, :]
    for f in range(3):
        for lev in range(levs):
            head[lev, f : f + 1, :] = head_rows[f, lev, 0:1, :]
    for lev in range(levs):
        head[lev, 3:4, :] = jnp.zeros((1, nlon), jnp.float32)

    def send(src, dst, c, to):
        return pltpu.make_async_remote_copy(
            src_ref=src, dst_ref=dst, send_sem=send_sem.at[c], recv_sem=recv_sem.at[c],
            device_id=(to, l), device_id_type=MESH,
        )

    pl.semaphore_wait(barrier, n_lat - 1 + n_lev - 1)

    @pl.when(i < n_lat - 1)
    def _():
        send(tail, south_ref, 0, i + 1).start()

    @pl.when(i > 0)
    def _():
        send(head, north_ref, 1, i - 1).start()

    @pl.when(i == 0)
    def _():
        south_ref[...] = jnp.zeros_like(south_ref)

    @pl.when(i == n_lat - 1)
    def _():
        north_ref[...] = jnp.zeros_like(north_ref)

    for copy in loads:
        copy.wait()

    @pl.when(i < n_lat - 1)
    def _():
        send(tail, south_ref, 0, i + 1).wait_send()
        send(head, north_ref, 1, i + 1).wait_recv()

    @pl.when(i > 0)
    def _():
        send(head, north_ref, 1, i - 1).wait_send()
        send(tail, south_ref, 0, i - 1).wait_recv()

    order = sorted(range(1, n_lat), key=lambda d: abs(d - n_lat / 2))
    per = n_lat // n_lev
    owner = i // per
    own_slot = l * per + i % per

    def remote(src, dst, ss, rs, dev):
        return pltpu.make_async_remote_copy(
            src_ref=src, dst_ref=dst, send_sem=ss, recv_sem=rs, device_id=dev, device_id_type=MESH
        )

    def stage1(d, c, direct):
        dst = out_ref.at[own_slot, c] if direct else mid.at[d, c]
        j = (i + d) % n_lat
        return remote(send_ref.at[j, c], dst, s1.at[d, c], r1.at[d, c], (j, l))

    def stage2(d, c, src_lat, src):
        slot = l * per + src_lat % per
        return remote(src, out_ref.at[slot, c], s2.at[d, c], r2.at[slot, c], (i, src_lat // per))

    def own_block(c):
        return pltpu.make_async_copy(send_ref.at[i, c], out_ref.at[own_slot, c], local.at[c])

    def sums_a(d):
        j = (i + d) % n_lat
        return remote(part_ref, sums_ref.at[l, i], sa.at[d], ra.at[d], (j, l))

    def sums_b(d):
        return remote(sums_ref.at[l], sums_ref.at[l], sb.at[d], rb.at[d], (i, (l + d) % n_lev))

    radix = nlon // LANES
    half = radix // 2
    first = pl.multiple_of(lax.axis_index("lat") * lats, SUB)
    table = rows_ref[pl.ds(first, lats), :]
    cc, icc, face, face_s = (table[:, c : c + 1] for c in range(4))
    face_s = face_s[0:1]
    row = lax.broadcasted_iota(jnp.int32, (lats, nlon), 0)

    def up(x, halo):
        return jnp.where(row == lats - 1, halo, pltpu.roll(x, lats - 1, 0))

    def down(x, halo):
        return jnp.where(row == 0, halo, pltpu.roll(x, 1, 0))

    def east(x):
        return pltpu.roll(x, nlon - 1, 1)

    def west(x):
        return pltpu.roll(x, 1, 1)

    clevs = levs // chunks
    sub_row = lax.broadcasted_iota(jnp.int32, (lats, 2 * LANES), 0)
    cuts = jnp.full((lats, 2 * LANES), nlon, jnp.int32)
    for r in range(lats):
        value = jnp.where(mask_ref[r] > 0, cut_ref[r], nlon)
        cuts = jnp.where(sub_row == r, value, cuts)
    k2 = lax.broadcasted_iota(jnp.int32, (lats, 2 * LANES), 1) % LANES

    dot = functools.partial(jnp.dot, preferred_element_type=jnp.float32)

    def dot_t(a, b):
        return lax.dot_general(a, b, (((1,), (1,)), ((), ())), preferred_element_type=jnp.float32)

    part_ref[...] = jnp.zeros_like(part_ref)

    for chunk in range(chunks):
        @pl.loop(0, clevs)
        def _(cl):
            l = cl + chunk * clevs
            p, t, q, ec, nc = (r[l] for r in (p_ref, t_ref, q_ref, e_ref, n_ref))
            em = ec * (p + east(p)) * 0.5
            nm = nc * (p + up(p, north_ref[l, 0:1])) * 0.5 * face
            sm = south_ref[l, 3:4] * (south_ref[l, 0:1] + p[0:1]) * 0.5 * face_s
            base = pl.multiple_of(cl * 3 * lats, SUB)
            tend[pl.ds(base, lats)] = -((em - west(em)) + (nm - down(nm, sm)) * icc)
            for f, s in ((1, t), (2, q)):
                es = em * (s + east(s)) * 0.5
                ns = nm * (s + up(s, north_ref[l, f : f + 1])) * 0.5
                ss = sm * (south_ref[l, f : f + 1] + s[0:1]) * 0.5
                tend[pl.ds(pl.multiple_of(base + f * lats, SUB), lats)] = -(
                    (es - west(es)) + (ns - down(ns, ss)) * icc
                )

        total_rows = tend.shape[0]
        block = 48 if total_rows % 48 == 0 else 16

        @pl.loop(0, total_rows // block)
        def _(rb):
            at = pl.ds(pl.multiple_of(rb * block, 16), block)
            c = [tend[at, a * LANES : (a + 1) * LANES] for a in range(radix)]
            s = [c[a] + c[radix - a] for a in range(1, half + 1)]
            d = [c[a] - c[radix - a] for a in range(1, half + 1)]
            for k1 in range(half + 1):
                re = c[0]
                im = None
                for a in range(1, half + 1):
                    angle = 2.0 * math.pi * (a * k1 % radix) / radix
                    re = re + s[a - 1] * math.cos(angle)
                    if k1:
                        term = d[a - 1] * -math.sin(angle)
                        im = term if im is None else im + term
                lo = 0 if k1 == 0 else LANES + (k1 - 1) * 2 * LANES
                h, w = split_bf16(re)
                yh[at, lo : lo + LANES] = h
                yl[at, lo : lo + LANES] = w
                if k1:
                    h, w = split_bf16(im)
                    yh[at, lo + LANES : lo + 2 * LANES] = h
                    yl[at, lo + LANES : lo + 2 * LANES] = w

        for k1 in range(half + 1):
            lo = 0 if k1 == 0 else LANES + (k1 - 1) * 2 * LANES
            size = LANES if k1 == 0 else 2 * LANES
            mh, ml = mh_ref[k1, :size], ml_ref[k1, :size]
            h, w = yh[:, lo : lo + size], yl[:, lo : lo + size]
            x = dot(h, mh) + dot(h, ml) + dot(w, mh)
            k = k1 + radix * k2
            wave = jnp.minimum(k, nlon - k)
            keep = jnp.where(wave >= cuts, (1.0 if k1 == 0 else 2.0) / nlon, 0.0)
            x = (x.reshape(-1, lats, 2 * LANES) * keep[None]).reshape(-1, 2 * LANES)
            h, w = split_bf16(x)
            spec[:, lo : lo + size] = dot_t(h, mh) + dot_t(h, ml) + dot_t(w, mh)

        @pl.loop(0, clevs)
        def _(cl):
            l = cl + chunk * clevs
            base = pl.multiple_of(cl * 3 * lats, SUB)

            def filtered(f):
                at = pl.ds(pl.multiple_of(base + f * lats, SUB), lats)
                z0 = spec[at, 0:LANES]
                re = [spec[at, (2 * k - 1) * LANES : 2 * k * LANES] for k in range(1, half + 1)]
                im = [spec[at, 2 * k * LANES : (2 * k + 1) * LANES] for k in range(1, half + 1)]
                parts = [None] * radix
                for a in range(half + 1):
                    even, odd = z0, None
                    for k in range(1, half + 1):
                        angle = 2.0 * math.pi * (a * k % radix) / radix
                        even = even + re[k - 1] * math.cos(angle)
                        if a:
                            term = im[k - 1] * math.sin(angle)
                            odd = term if odd is None else odd + term
                    if a:
                        parts[a] = even - odd
                        parts[radix - a] = even + odd
                    else:
                        parts[0] = even
                return tend[at] - jnp.concatenate(parts, axis=1)

            p, t, q = p_ref[l], t_ref[l], q_ref[l]
            fm = filtered(0)
            np_ = p + fm
            inv = 1.0 / p
            new[pl.ds(base, lats)] = np_
            area = np_ * cc
            acc = part_ref[...]
            for g in range(lats // SUB):
                for a in range(radix):
                    acc = acc + area[g * SUB : (g + 1) * SUB, a * LANES : (a + 1) * LANES]
            part_ref[...] = acc
            for f, s in ((1, t), (2, q)):
                new[pl.ds(pl.multiple_of(base + f * lats, SUB), lats)] = s + (filtered(f) - s * fm) * inv

        width = nlon // n_lat
        groups = total_rows // SUB
        full, rest, cap, tail_tiles = pack_plan(width, groups)
        lane = lax.broadcasted_iota(jnp.int32, (SUB, LANES), 1)
        for j in range(n_lat):
            t0, off = divmod(width * j, LANES)
            nt = -(-(off + width) // LANES)
            acc = None
            for g in range(groups):
                def piece(a):
                    t, cut = divmod(width * j + a * LANES, LANES)
                    wide = LANES if a < full else rest
                    at = slice(g * SUB, (g + 1) * SUB)
                    x = new[at, t * LANES : (t + 1) * LANES]
                    if cut + wide > LANES:
                        y = new[at, (t + 1) * LANES : (t + 2) * LANES]
                        x = jnp.where(lane >= cut, x, y)
                    return x

                for a in range(full):
                    o = (a * groups + g) * SUB
                    send_ref[j, chunk, o : o + SUB, :] = piece(a)
                if rest:
                    slot = g % cap
                    y = piece(full)
                    if (slot * rest - off) % LANES:
                        y = pltpu.roll(y, (slot * rest - off) % LANES, 1)
                    acc = y if slot == 0 else jnp.where(lane >= slot * rest, y, acc)
                    if slot == cap - 1 or g == groups - 1:
                        o = (full * groups + g // cap) * SUB
                        send_ref[j, chunk, o : o + SUB, :] = acc


        @pl.when(owner == l)
        def _():
            for d in order:
                stage1(d, chunk, True).start()
            own_block(chunk).start()

        @pl.when(owner != l)
        def _():
            for d in order:
                stage1(d, chunk, False).start()
            stage2(0, chunk, i, send_ref.at[i, chunk]).start()


    own_part = pltpu.make_async_copy(part_ref, sums_ref.at[l, i], local.at[chunks])
    own_part.start()
    for d in order:
        sums_a(d).start()
    for c in range(chunks):
        for d in order:
            src_lat = (i + n_lat - d) % n_lat
            stage1(d, c, False).wait_recv()

            @pl.when(src_lat // per != l)
            def _():
                stage2(d, c, src_lat, mid.at[d, c]).start()

        if c == 0:
            own_part.wait()
            for d in order:
                sums_a(d).wait_recv()
            for d in range(1, n_lev):
                sums_b(d).start()

    for e in range(1, n_lev):
        for r in range(per):
            slot = ((l + e) % n_lev) * per + r
            for c in range(chunks):
                remote(mid.at[0, c], out_ref.at[slot, c], s2.at[0, c], r2.at[slot, c], (i, l)).wait_recv()
    for d in range(1, n_lev):
        sums_b(d).wait_recv()

    for d in order:
        sums_a(d).wait_send()
        src_lat = (i + n_lat - d) % n_lat
        for c in range(chunks):
            stage1(d, c, False).wait_send()

        @pl.when(src_lat // per != l)
        def _():
            for c in range(chunks):
                stage2(d, c, src_lat, mid.at[d, c]).wait_send()

    for d in range(1, n_lev):
        sums_b(d).wait_send()

    @pl.when(owner == l)
    def _():
        for c in range(chunks):
            own_block(c).wait()

    @pl.when(owner != l)
    def _():
        for c in range(chunks):
            stage2(0, c, i, send_ref.at[i, c]).wait_send()


def remap_kernel(
    n_lat, n_lev, chunks, lats, nlon, area_total,
    got_hbm, sums_ref, weight_ref, target_ref,
    thick_out, temp_out, tracer_out,
    cols, share, res, got, thick_buf, temp_buf, tracer_buf, in_sem, out_sem,
):
    per = n_lat // n_lev
    levels = thick_out.shape[0]
    levs = levels // n_lev
    rgs = lats // SUB
    width = nlon // n_lat
    clevs = levs // chunks
    groups = clevs * 3 * rgs
    full, rest, cap, tail_tiles = pack_plan(width, groups)
    lane = lax.broadcasted_iota(jnp.int32, (SUB, LANES), 1)
    outs = (thick_buf, temp_buf, tracer_buf)
    turn = (LANES - lax.axis_index("lat") * width % LANES) % LANES
    finals = (thick_out, temp_out, tracer_out)
    loads = [
        pltpu.make_async_copy(got_hbm.at[slot], got.at[slot], in_sem.at[slot])
        for slot in range(n_lev * per)
    ]
    for copy in loads:
        copy.start()

    whole = jnp.full((SUB, LANES), weight_ref[0])
    for k in range(1, levels):
        whole = whole + weight_ref[k]
    run = jnp.zeros((SUB, LANES), jnp.float32)
    for k in range(levels):
        part = jnp.full((SUB, LANES), weight_ref[k]) / whole
        run = run + part
        share[0, k] = part
        share[1, k] = run
        share[2, k] = 1.0 / part
    sums = sums_ref[...].reshape(-1, SUB, LANES)
    total = jnp.sum(jnp.sum(sums, axis=0), keepdims=True)
    factor = jnp.full((1, 1), target_ref[0] * (nlon * area_total)) / total

    n_main = full * per * rgs
    col_groups = per * rgs
    for lev in range(n_lev):
        for rs in range(per):
            loads[lev * per + rs].wait()
        for ll in range(levs):
            c, cl = divmod(ll, clevs)
            for f in range(3):
                acc = None
                for rs in range(per):
                    for rg in range(rgs):
                        g = (cl * 3 + f) * rgs + rg
                        for a in range(full):
                            v = (a * per + rs) * rgs + rg
                            o = (a * groups + g) * SUB
                            cols[f, lev * levs + ll, v] = got[lev * per + rs, c, o : o + SUB, :]
                        if rest:
                            o = (full * groups + g // cap) * SUB
                            y = got[lev * per + rs, c, o : o + SUB, :]
                            cg = rs * rgs + rg
                            slot = cg % cap
                            shift = (slot - g % cap) * rest % LANES
                            if shift:
                                y = pltpu.roll(y, shift, 1)
                            acc = (
                                y if slot == 0
                                else jnp.where(lane >= slot * rest, y, acc)
                            )
                            if slot == cap - 1 or cg == col_groups - 1:
                                last = (slot + 1) * rest
                                if last < LANES:
                                    acc = jnp.where(lane < last, acc, 1.0)
                                cols[f, lev * levs + ll, n_main + cg // cap] = acc

    def remap(v, put):
        thick = [cols[0, m, v] for m in range(levels)]
        tops = []
        surface = jnp.zeros((SUB, LANES), jnp.float32)
        for m in range(levels):
            tops.append(surface)
            surface = surface + thick[m]
        inv = 1.0 / surface
        scale = surface * factor
        before = (jnp.zeros_like(surface), jnp.zeros_like(surface))
        for k in range(levels):
            bound = surface * share[1, k]
            ct = cq = None
            for m in range(levels):
                w = jnp.minimum(jnp.maximum(bound - tops[m], 0.0), thick[m])
                dt, dq = cols[1, m, v] * w, cols[2, m, v] * w
                ct, cq = (dt, dq) if m == 0 else (ct + dt, cq + dq)
            per_share = inv * share[2, k]
            put(k, scale * share[0, k], (ct - before[0]) * per_share, (cq - before[1]) * per_share)
            before = (ct, cq)

    if rest:
        n_tail = -(-col_groups // cap)

        @pl.loop(0, n_tail)
        def _(v):
            def put(k, *values):
                for f, x in enumerate(values):
                    res[f, k, v] = x

            remap(n_main + v, put)

        for cg in range(col_groups):
            @pl.loop(0, levels)
            def _(k):
                for f in range(3):
                    x = res[f, k, cg // cap]
                    if cg % cap:
                        x = pltpu.roll(x, LANES - (cg % cap) * rest, 1)
                    outs[f][k, cg * SUB : (cg + 1) * SUB, full * LANES : full * LANES + rest] = x[:, :rest]

    def finish(v):
        at = pl.ds(pl.multiple_of(v * SUB, SUB), SUB)
        return [
            pltpu.make_async_copy(outs[f].at[:, at, :], finals[f].at[:, at, :], out_sem.at[f, v])
            for f in range(3)
        ]

    for a in range(full):
        @pl.loop(0, col_groups)
        def _(v):
            at = pl.ds(pl.multiple_of(v * SUB, SUB), SUB)

            def put(k, *values):
                for ref, x in zip(outs, values):
                    x = pltpu.roll(x, turn, 1)
                    ref[k, at, a * LANES : (a + 1) * LANES] = x

            remap(a * col_groups + v, put)
            if a == full - 1:
                for copy in finish(v):
                    copy.start()

    if not full:
        for v in range(col_groups):
            for copy in finish(v):
                copy.start()
    for v in range(col_groups):
        for copy in finish(v):
            copy.wait()


def on_device(p, t, q, ec, nc, polar_mask, wave_cutoff, level_weight, target_surface):
    levs, lats, nlon = p.shape
    n_lat, n_lev = lax.axis_size("lat"), lax.axis_size("lev")
    nlat = lats * n_lat
    levels = levs * n_lev
    per = n_lat // n_lev
    width = nlon // n_lat
    f32 = jnp.float32
    high, low = dft_tables(nlon)
    chunks = 2
    rows = levs * 3 * lats
    crows = rows // chunks
    groups = crows // SUB
    full, rest, cap, tail_tiles = pack_plan(width, groups)
    packed = (full * groups + tail_tiles) * SUB
    dma = pltpu.SemaphoreType.DMA
    grant = 62_800_000
    given = (p, t, q, ec, nc, jnp.asarray(row_tables(nlat)), jnp.asarray(high), jnp.asarray(low))
    hbm = pl.BlockSpec(memory_space=pltpu.HBM)
    got, sums = pl.pallas_call(
        functools.partial(step_kernel, n_lat, n_lev, chunks),
        out_shape=(
            jax.ShapeDtypeStruct((n_lat, chunks, packed, LANES), f32),
            jax.ShapeDtypeStruct((n_lev, n_lat, SUB, LANES), f32),
        ),
        in_specs=[hbm] * 8 + [SMEM] * 2,
        out_specs=(hbm, hbm),
        scratch_shapes=[pltpu.VMEM(x.shape, x.dtype) for x in given] + [
            pltpu.VMEM((4, levs, SUB, nlon), f32),
            pltpu.VMEM((3, levs, SUB, nlon), f32),
            pltpu.VMEM((levs, 4, nlon), f32),
            pltpu.VMEM((levs, 4, nlon), f32),
            pltpu.VMEM((levs, 4, nlon), f32),
            pltpu.VMEM((levs, 4, nlon), f32),
            pltpu.VMEM((crows, nlon), f32),
            pltpu.VMEM((crows, nlon), f32),
            pltpu.VMEM((crows, nlon), f32),
            pltpu.VMEM((crows, nlon), jnp.bfloat16),
            pltpu.VMEM((crows, nlon), jnp.bfloat16),
            pltpu.VMEM((n_lat, chunks, packed, LANES), f32),
            pltpu.VMEM((SUB, LANES), f32),
            pltpu.VMEM((n_lat, chunks, packed, LANES), f32),
            dma((8,)), dma((2, 4)), dma((2,)), dma((2,)),
            dma((n_lat, chunks)), dma((n_lat, chunks)), dma((n_lat, chunks)), dma((n_lat, chunks)),
            dma((chunks + 1,)), dma((n_lat,)), dma((n_lat,)), dma((n_lev,)), dma((n_lev,)),
        ],
        compiler_params=pltpu.CompilerParams(
            collective_id=0, has_side_effects=True, vmem_limit_bytes=grant
        ),
        name="step",
    )(*given, polar_mask, wave_cutoff)

    area_total = float(np.sum(np.sin((np.arange(nlat) + 0.5) * np.pi / nlat)))
    col_groups = per * lats // SUB
    n_tail = -(-col_groups // cap) if rest else 0
    out = jax.ShapeDtypeStruct((levels, nlat // n_lev, width), f32)
    return pl.pallas_call(
        functools.partial(remap_kernel, n_lat, n_lev, chunks, lats, nlon, area_total),
        out_shape=(out, out, out),
        in_specs=[hbm, VMEM, SMEM, SMEM],
        out_specs=(hbm, hbm, hbm),
        scratch_shapes=[
            pltpu.VMEM((3, levels, full * col_groups + n_tail, SUB, LANES), f32),
            pltpu.VMEM((3, levels, SUB, LANES), f32),
            pltpu.VMEM((3, levels, max(n_tail, 1), SUB, LANES), f32),
            pltpu.VMEM(got.shape, f32),
            pltpu.VMEM(out.shape, f32), pltpu.VMEM(out.shape, f32), pltpu.VMEM(out.shape, f32),
            dma((n_lat,)), dma((3, col_groups)),
        ],
        compiler_params=pltpu.CompilerParams(vmem_limit_bytes=grant),
        name="remap",
    )(got, sums, level_weight, target_surface)


def solution(mesh):
    return jax.shard_map(
        on_device,
        mesh=mesh,
        in_specs=(P("lev", "lat", None),) * 5 + (P("lat"), P("lat"), P(), P()),
        out_specs=(P(None, "lev", "lat"),) * 3,
        check_vma=False,
    )
```
